32 devices in a mesh: group: 2 (over y), seq: 8 (over z, x), tensor: 2 (over core).
Axes of the slice: x: 2, y: 2, z: 4, core: 2. Of those that a mesh axis runs over, the one named last changes fastest.
Arguments:
- query: bfloat16 [32, 64, 128], P('group', 'tensor'), parts along dimension 0, may hold values from -400 to 400
- key_cache: bfloat16 [512, 128, 8, 128], P(('group', 'seq'), None, 'tensor'), parts along dimension 0, may hold values from -6 to 6
- value_cache: bfloat16 [512, 128, 8, 128], P(('group', 'seq'), None, 'tensor'), parts along dimension 0, may hold values from -6 to 6
- lengths: int32 [32], P('group'), parts along dimension 0, may hold values from 1 to 8192, 14336 in all
- page_order: int32 [512], P('group'), parts along dimension 0, may hold values from 0 to 255, as said below
- out_weight: bfloat16 [8192, 8192], P('tensor', 'seq'), may hold values from -0.59765625 to 0.59765625
Outputs:
- mixed: bfloat16 [32, 8192], P(('group', 'tensor'), 'seq'), parts along dimension 0
The draws below stay inside these ranges and needn't reach their ends.
There are 2 independent parts, one for each index of `group`. The reference program is written for one: setup_inputs(seed, part) draws one part's arguments, and reference() takes and returns one part's arrays. A program takes and returns all parts, laid end to end along the dimension named above; an argument that names none is the same for every part. Nothing has to cross between parts.
Inputs may be any that keep to these rules, and one draw needn't show every extreme that they name: The sequences' lengths sum to 14336; one equals 8192. `page_order`: a permutation of the pages.
All inputs are finite; a program needn't handle non-finite values.
Results may differ from the reference program's by a relative error of at most 0.0065.
Values may be sent and summed in bfloat16 or wider, within the bound.
A program may use at most 64 MiB of HBM per device.

```python
import math
import jax
import jax.numpy as jnp
import numpy as np
from jax import lax

D = 8192
HEADS = 64
KVH = 8
HD = 128
PAGE = 128
PAGES_DEV = 32
SEQS = 16
POOL = 256
MAXBLK = 64
MAXLEN = 8192
TOTAL = 14336


def draw_key_cache(key, part):
    cached = jax.random.truncated_normal(jax.random.fold_in(key, 21), -6.0, 6.0, (POOL, PAGE, KVH, HD), jnp.float32)
    return cached.astype(jnp.bfloat16)


def draw_query(key, part):
    queries = 1.5 * jax.random.truncated_normal(jax.random.fold_in(key, 31), -4.0, 4.0, (SEQS, HEADS, HD), jnp.float32)
    return queries.astype(jnp.bfloat16)


def draw_page_order(key, part):
    noise = jax.random.randint(jax.random.fold_in(key, 51), (POOL,), 0, 65536)
    page_bias = jax.random.randint(jax.random.fold_in(key, 52), (POOL // PAGES_DEV,), 0, 3)
    device_bias = jnp.repeat(page_bias, PAGES_DEV)
    sort_score = (device_bias * 65536 + noise) * POOL + jnp.arange(POOL, dtype=jnp.int32)
    return jnp.argsort(sort_score, stable=True).astype(jnp.int32)


def block_levels(own_key, shape, split, low, high):
    gain = 1.0
    for axis_at, blocks in split:
        draws = jax.random.uniform(jax.random.fold_in(jax.random.fold_in(own_key, 6), axis_at), (blocks,), jnp.float32, low / len(split), high / len(split))
        gain = gain * jnp.repeat(jnp.exp(draws), shape[axis_at] // blocks).reshape((-1,) + (1,) * (len(shape) - 1 - axis_at))
    return gain


def length_profile(count, total, reach, skew):
    portions = [(1 << 20) // math.isqrt(grade ** skew) + 1 for grade in range(2, count + 1)]
    rest, given = total - reach - (count - 1), [1] * (count - 1)
    while rest > 0:
        free = [i for i in range(count - 1) if given[i] < reach]
        whole, budget = sum([portions[i] for i in free]), rest
        for i in free:
            more = min(reach - given[i], max(1, budget * portions[i] // whole), rest)
            given[i] = given[i] + more
            rest = rest - more
    return np.array([reach] + given)


def ragged(stream_key, amount, total, reach, skew):
    if amount == 2:
        one = jax.random.randint(stream_key, (), max(1, total - reach), min(reach, total - 1) + 1)
        return jnp.stack([one, total - one])
    sizes = jnp.asarray(length_profile(amount, total, reach, skew), jnp.int32)
    pairs = (amount - 1) // 2
    donor, sink = sizes[1:1 + 2 * pairs:2], sizes[2:2 + 2 * pairs:2]
    room = jnp.minimum(donor - 1, reach - sink)
    shifted = jax.random.randint(jax.random.fold_in(stream_key, 1), (pairs,), 0, 1 << 20) % (room + 1)
    sizes = sizes.at[1:1 + 2 * pairs:2].set(donor - shifted).at[2:2 + 2 * pairs:2].set(sink + shifted)
    return sizes[jax.random.permutation(jax.random.fold_in(stream_key, 2), amount)]


def bell_draw(rng, dims, width, bound, cuts=(), kind=jnp.bfloat16):
    result = width * jax.random.normal(rng, dims, jnp.float32)
    if cuts:
        result = result * block_levels(rng, dims, cuts, -0.22, 0.18)
    return jnp.clip(result, -bound, bound).astype(kind)


def setup_inputs(seed: int = 0, part: int = 0) -> dict:
    seeds = jax.random.split(jax.random.key(seed), 7)
    part_splits = jax.random.split(jax.random.fold_in(seeds[6], part), 7)
    query = draw_query(jax.random.fold_in(jax.random.fold_in(seeds[6], part), 71), part)
    key_cache = draw_key_cache(jax.random.fold_in(jax.random.fold_in(seeds[6], part), 71), part)
    value_cache = bell_draw(part_splits[2], (POOL, PAGE, KVH, HD), 1.0, 6.0, ((0, 8), (2, 2)))
    lengths = ragged(part_splits[3], SEQS, TOTAL, MAXLEN, 2).astype(jnp.int32)
    page_order = draw_page_order(jax.random.fold_in(jax.random.fold_in(seeds[6], part), 71), part)
    out_weight = bell_draw(seeds[5], (HEADS * HD, D), 0.1, 0.59765625, ((0, 2), (1, 8)))
    return dict(query=query, key_cache=key_cache, value_cache=value_cache, lengths=lengths, page_order=page_order, out_weight=out_weight)


def reference(query, key_cache, value_cache, lengths, page_order, out_weight):
    counts = (lengths + PAGE - 1) // PAGE
    starts = (jnp.cumsum(counts) - counts).astype(jnp.int32)
    group_size = HEADS // KVH
    score_scale = 1.0 / math.sqrt(HD)

    def per_sequence(inputs):
        seq_query, seq_length, seq_start = inputs
        page_slots = jnp.clip(seq_start + jnp.arange(MAXBLK, dtype=jnp.int32), 0, POOL - 1).astype(jnp.int32)
        page_ids = page_order[page_slots]
        seq_keys = key_cache[page_ids].astype(jnp.float32)
        seq_values = value_cache[page_ids].astype(jnp.float32)
        grouped = seq_query.astype(jnp.float32).reshape(KVH, group_size, HD)
        scores = jnp.einsum('ghd,ptgd->pght', grouped, seq_keys, precision=lax.Precision.HIGHEST) * score_scale
        positions = jnp.arange(MAXBLK, dtype=jnp.int32)[:, None] * PAGE + jnp.arange(PAGE, dtype=jnp.int32)[None, :]
        is_valid = (positions < seq_length)[:, None, None, :]
        scores = jnp.where(is_valid, scores, -1e+30)
        block_max = lax.optimization_barrier(jnp.max(scores, axis=-1))
        weights = jnp.where(is_valid, jnp.exp(scores - block_max[..., None]), 0.0).astype(jnp.bfloat16)
        wide_weights = weights.astype(jnp.float32)
        block_sum = lax.optimization_barrier(jnp.sum(wide_weights, axis=-1))
        block_out = jnp.einsum('pght,ptgd->pghd', wide_weights, seq_values, precision=lax.Precision.HIGHEST)
        largest = lax.optimization_barrier(jnp.max(block_max, axis=0))
        factor = jnp.exp(block_max - largest)
        denominator = lax.optimization_barrier(jnp.sum(factor * block_sum, axis=0))
        numerator = lax.optimization_barrier(jnp.sum(factor[..., None] * block_out, axis=0))
        return (numerator / denominator[..., None]).reshape(HEADS * HD).astype(jnp.bfloat16)
    attended = lax.map(per_sequence, (query, lengths, starts))
    return jnp.dot(attended, out_weight, preferred_element_type=jnp.float32).astype(jnp.bfloat16)
```

```python
import functools
import math

import jax
import jax.numpy as jnp
from jax import lax
from jax.experimental import pallas as pl
from jax.experimental.pallas import tpu as pltpu
from jax.sharding import PartitionSpec as P

MASKED = -1e30
FLOOR = -1e29
LANES = 128
MESH = pl.DeviceIdType.MESH


def attend_kernel(
    page_len,
    group_size,
    chunk,
    exponent_scale,
    lengths_ref,
    order_ref,
    query_ref,
    key_hbm,
    value_hbm,
    out_ref,
    stats_ref,
    keys,
    values,
    scores,
    meta_vector,
    meta,
    top,
    total,
    gathered,
    by_head,
    key_sems,
    value_sems,
    meta_sem,
):
    pages, rows, head_dim = keys.shape
    seqs, heads, _ = query_ref.shape
    kv_local = rows // page_len
    shards, shard_rows, _ = out_ref.shape
    chunks = pages // chunk

    def key_copy(c):
        part = pl.ds(c * chunk, chunk)
        return pltpu.make_async_copy(key_hbm.at[part], keys.at[part], key_sems.at[c])

    def value_copy(c):
        part = pl.ds(c * chunk, chunk)
        return pltpu.make_async_copy(value_hbm.at[part], values.at[part], value_sems.at[c])

    for c in range(chunks):
        key_copy(c).start()
    for c in range(chunks):
        value_copy(c).start()

    pool = order_ref.shape[0]
    order = order_ref[...].reshape(1, pool)
    rank = lax.broadcasted_iota(jnp.int32, (1, pool), 1)
    owner_row = jnp.zeros((1, pool), jnp.int32)
    limit_row = jnp.zeros((1, pool), jnp.int32)
    start = jnp.int32(0)
    for s in range(seqs):
        length = lengths_ref[s]
        reached = rank >= start
        owner_row = jnp.where(reached, s, owner_row)
        limit_row = jnp.where(reached, length + start * page_len, limit_row)
        start = start + lax.div(length + (page_len - 1), page_len)
    valid_row = jnp.clip(limit_row - rank * page_len, 0, page_len)
    packed = (owner_row * (2 * page_len) + valid_row).astype(jnp.float32)
    local_page = lax.axis_index("seq") * pages + lax.broadcasted_iota(jnp.int32, (pages, pool), 0)
    found = jnp.sum(jnp.where(order == local_page, packed, 0.0), axis=1, keepdims=True)
    meta_vector[...] = jnp.broadcast_to(found, (pages, LANES)).astype(jnp.int32)
    meta_copy = pltpu.make_async_copy(meta_vector, meta, meta_sem)
    meta_copy.start()

    top[...] = jnp.full(top.shape, FLOOR, jnp.float32)
    total[...] = jnp.zeros(total.shape, jnp.float32)
    gathered[...] = jnp.zeros(gathered.shape, jnp.float32)
    column = lax.broadcasted_iota(jnp.int32, (heads, rows), 1)
    row_head = lax.broadcasted_iota(jnp.int32, (heads, rows), 0) // group_size
    column_limit = jnp.where(column % kv_local == row_head, column, rows)
    meta_copy.wait()

    def owner_of(p):
        return lax.div(meta[p, 0], 2 * page_len)

    @pl.loop(0, chunks)
    def _(c):
        key_copy(c).wait()
        for i in range(chunk):
            p = c * chunk + i
            owner = owner_of(p)
            count = lax.rem(meta[p, 0], 2 * page_len) * kv_local
            score = lax.dot_general(
                query_ref[owner],
                keys[p],
                (((1,), (1,)), ((), ())),
                preferred_element_type=jnp.float32,
            )
            score = jnp.where(column_limit < count, score, MASKED)
            scores[p] = score
            block_max = jnp.max(score, axis=1, keepdims=True)
            top[owner] = jnp.maximum(top[owner], jnp.broadcast_to(block_max, (heads, LANES)))

    @pl.loop(0, chunks)
    def _(c):
        value_copy(c).wait()
        for i in range(chunk):
            p = c * chunk + i
            owner = owner_of(p)
            highest = jnp.concatenate([top[owner]] * (rows // LANES), axis=1)
            weight = jnp.exp2((scores[p] - highest) * exponent_scale).astype(jnp.bfloat16)
            wide = weight.astype(jnp.float32)
            partial = wide[:, :LANES]
            for b in range(1, rows // LANES):
                partial = partial + wide[:, b * LANES : (b + 1) * LANES]
            total[owner] = total[owner] + partial
            gathered[owner] = gathered[owner] + jnp.dot(
                weight, values[p], preferred_element_type=jnp.float32
            )

    for s in range(seqs):
        where = pl.ds(s, heads, stride=seqs)
        by_head[0, where, :] = gathered[s]
        by_head[1, where, :] = top[s]
        by_head[2, where, :] = jnp.broadcast_to(
            jnp.sum(total[s], axis=1, keepdims=True), (heads, LANES)
        )
    out_ref[...] = by_head[0].reshape(shards, shard_rows, head_dim).astype(out_ref.dtype)
    diagonal = lax.broadcasted_iota(jnp.int32, (shard_rows, LANES), 0) == (
        lax.broadcasted_iota(jnp.int32, (shard_rows, LANES), 1)
    )
    for j in range(shards):
        for k in range(2):
            part = by_head[1 + k, j * shard_rows : (j + 1) * shard_rows, :]
            stats_ref[j, k : k + 1, :] = jnp.sum(
                jnp.where(diagonal, part, 0.0), axis=0, keepdims=True
            )


def mix_kernel(
    seqs,
    exponent_scale,
    partial_ref,
    stats_ref,
    weight_hbm,
    out_ref,
    outs_in,
    stats_in,
    attended,
    weight,
    sums,
    sums_in,
    weight_sems,
    out_send,
    out_recv,
    stats_send,
    stats_recv,
    att_send,
    att_recv,
    sum_send,
    sum_recv,
):
    shards, shard_rows, head_dim = partial_ref.shape
    ways = sums.shape[0]
    me = lax.axis_index("seq")
    half = lax.axis_index("tensor")
    pieces = weight_sems.shape[0]
    depth = weight.shape[0] // pieces
    loads = []
    for c in range(pieces):
        part = pl.ds(c * depth, depth)
        loads.append(
            pltpu.make_async_copy(weight_hbm.at[part], weight.at[part], weight_sems.at[c])
        )

    barrier = pltpu.get_barrier_semaphore()
    for k in range(1, shards):
        pl.semaphore_signal(
            barrier, inc=1, device_id={"seq": lax.rem(me + k, shards)}, device_id_type=MESH
        )
    for k in range(1, ways):
        pl.semaphore_signal(
            barrier, inc=1, device_id={"tensor": lax.rem(half + k, ways)}, device_id_type=MESH
        )
    for load in loads:
        load.start()
    pl.semaphore_wait(barrier, shards + ways - 2)

    sends = []
    for k in range(1, shards):
        peer = lax.rem(me + k, shards)
        for source, target, send, recv in (
            (stats_ref, stats_in, stats_send, stats_recv),
            (partial_ref, outs_in, out_send, out_recv),
        ):
            copy = pltpu.make_async_remote_copy(
                src_ref=source.at[peer],
                dst_ref=target.at[k],
                send_sem=send.at[k],
                recv_sem=recv.at[k],
                device_id={"seq": peer},
                device_id_type=MESH,
            )
            copy.start()
            sends.append(copy)
    stats_in[0] = stats_ref[me]
    for copy in sends[0::2]:
        copy.wait_recv()
    tops = jnp.concatenate([stats_in[k, 0:1, :] for k in range(shards)], axis=0)
    totals = jnp.concatenate([stats_in[k, 1:2, :] for k in range(shards)], axis=0)
    factor = jnp.exp2((tops - jnp.max(tops, axis=0, keepdims=True)) * exponent_scale)
    denominator = jnp.sum(factor * totals, axis=0, keepdims=True)
    used = lax.broadcasted_iota(jnp.int32, (1, LANES), 1) < shard_rows
    share = factor / jnp.where(used, denominator, 1.0)
    diagonal = lax.broadcasted_iota(jnp.int32, (shard_rows, LANES), 0) == (
        lax.broadcasted_iota(jnp.int32, (shard_rows, LANES), 1)
    )

    def column(k):
        return jnp.sum(jnp.where(diagonal, share[k : k + 1, :], 0.0), axis=1, keepdims=True)

    columns = [column(k) for k in range(shards)]
    mine = columns[0] * partial_ref[me].astype(jnp.float32)
    for k in range(1, shards):
        sends[2 * k - 1].wait_recv()
        mine = mine + columns[k] * outs_in[k].astype(jnp.float32)
    attended[me] = mine.astype(jnp.bfloat16)

    gathers = []
    for k in range(1, shards):
        copy = pltpu.make_async_remote_copy(
            src_ref=attended.at[me],
            dst_ref=attended.at[me],
            send_sem=att_send.at[k],
            recv_sem=att_recv.at[k],
            device_id={"seq": lax.rem(me + k, shards)},
            device_id_type=MESH,
        )
        copy.start()
        gathers.append(copy)
    for load in loads:
        load.wait()

    whole_heads = shard_rows // seqs
    if shard_rows % seqs == 0:
        span = whole_heads * head_dim
        result = None
        for k in range(shards):
            source = lax.rem(me + shards - k, shards)
            if k:
                pltpu.make_async_remote_copy(
                    src_ref=attended.at[source],
                    dst_ref=attended.at[source],
                    send_sem=att_send.at[k],
                    recv_sem=att_recv.at[k],
                    device_id={"seq": lax.rem(me + k, shards)},
                    device_id_type=MESH,
                ).wait_recv()
            block = attended[source]
            left = jnp.concatenate(
                [block[h * seqs : (h + 1) * seqs] for h in range(whole_heads)], axis=1
            )
            rows = weight[pl.ds(pl.multiple_of(source * span, span), span), :]
            product = jnp.dot(left, rows, preferred_element_type=jnp.float32)
            result = product if result is None else result + product
    else:
        for k in range(1, shards):
            gathers[k - 1].wait_recv()
        per_head = seqs // shard_rows
        result = None
        for h in range(shards // per_head):
            left = jnp.concatenate(
                [attended[h * per_head + i].astype(jnp.float32) for i in range(per_head)], axis=0
            ).astype(jnp.bfloat16)
            product = jnp.dot(
                left,
                weight[h * head_dim : (h + 1) * head_dim, :],
                preferred_element_type=jnp.float32,
            )
            result = product if result is None else result + product

    kept = seqs // ways
    for i in range(ways):
        sums[i] = result[i * kept : (i + 1) * kept]
    shares = []
    for k in range(1, ways):
        peer = lax.rem(half + k, ways)
        copy = pltpu.make_async_remote_copy(
            src_ref=sums.at[peer],
            dst_ref=sums_in.at[k - 1],
            send_sem=sum_send.at[k],
            recv_sem=sum_recv.at[k],
            device_id={"tensor": peer},
            device_id_type=MESH,
        )
        copy.start()
        shares.append(copy)
    mixed = sums[half]
    for k in range(1, ways):
        shares[k - 1].wait_recv()
        mixed = mixed + sums_in[k - 1]
    out_ref[...] = mixed.astype(out_ref.dtype)
    for copy in sends + gathers + shares:
        copy.wait_send()


def body(shards, ways, query, key_cache, value_cache, lengths, page_order, out_weight):
    pages, page_len, kv_local, head_dim = key_cache.shape
    seqs, heads, _ = query.shape
    rows = page_len * kv_local
    shard_rows = seqs * heads // shards
    chunk = 4
    exponent_scale = math.log2(math.e) / math.sqrt(head_dim)
    vmem = pl.BlockSpec(memory_space=pltpu.VMEM)
    smem = pl.BlockSpec(memory_space=pltpu.SMEM)
    hbm = pl.BlockSpec(memory_space=pl.ANY)
    f32, bf16 = jnp.float32, jnp.bfloat16
    dma = pltpu.SemaphoreType.DMA

    partial, stats = pl.pallas_call(
        functools.partial(attend_kernel, page_len, heads // kv_local, chunk, exponent_scale),
        out_shape=(
            jax.ShapeDtypeStruct((shards, shard_rows, head_dim), bf16),
            jax.ShapeDtypeStruct((shards, 2, LANES), f32),
        ),
        in_specs=[smem, vmem, vmem, hbm, hbm],
        out_specs=(vmem, vmem),
        scratch_shapes=[
            pltpu.VMEM((pages, rows, head_dim), bf16),
            pltpu.VMEM((pages, rows, head_dim), bf16),
            pltpu.VMEM((pages, heads, rows), f32),
            pltpu.VMEM((pages, LANES), jnp.int32),
            pltpu.SMEM((pages, LANES), jnp.int32),
            pltpu.VMEM((seqs, heads, LANES), f32),
            pltpu.VMEM((seqs, heads, LANES), f32),
            pltpu.VMEM((seqs, heads, head_dim), f32),
            pltpu.VMEM((3, seqs * heads, LANES), f32),
            dma((pages // chunk,)),
            dma((pages // chunk,)),
            dma,
        ],
    )(
        lengths,
        page_order,
        query,
        key_cache.reshape(pages, rows, head_dim),
        value_cache.reshape(pages, rows, head_dim),
    )

    depth, width = out_weight.shape
    kept = seqs // ways
    return pl.pallas_call(
        functools.partial(mix_kernel, seqs, exponent_scale),
        out_shape=jax.ShapeDtypeStruct((kept, width), bf16),
        in_specs=[vmem, vmem, hbm],
        out_specs=vmem,
        scratch_shapes=[
            pltpu.VMEM((shards, shard_rows, head_dim), bf16),
            pltpu.VMEM((shards, 2, LANES), f32),
            pltpu.VMEM((shards, shard_rows, head_dim), bf16),
            pltpu.VMEM((depth, width), bf16),
            pltpu.VMEM((ways, kept, width), f32),
            pltpu.VMEM((max(ways - 1, 1), kept, width), f32),
            dma((8,)),
            dma((shards,)),
            dma((shards,)),
            dma((shards,)),
            dma((shards,)),
            dma((shards,)),
            dma((shards,)),
            dma((ways,)),
            dma((ways,)),
        ],
        compiler_params=pltpu.CompilerParams(collective_id=0, has_side_effects=True),
    )(partial, stats, out_weight)


def solution(mesh):
    in_specs = (
        P("group", "tensor", None),
        P(("group", "seq"), None, "tensor", None),
        P(("group", "seq"), None, "tensor", None),
        P("group"),
        P("group"),
        P("tensor", "seq"),
    )
    out_specs = P(("group", "tensor"), "seq")
    step = functools.partial(body, mesh.shape["seq"], mesh.shape["tensor"])
    return jax.shard_map(step, mesh=mesh, in_specs=in_specs, out_specs=out_specs, check_vma=False)
```

```python
import functools
import math

import jax
import jax.numpy as jnp
from jax import lax
from jax.experimental import pallas as pl
from jax.experimental.pallas import tpu as pltpu
from jax.sharding import PartitionSpec as P

MASKED = -1e30
FLOOR = -1e29
LANES = 128
UNROLL = 8
MESH = pl.DeviceIdType.MESH


def attend(
    page_len,
    group_size,
    chunk,
    step,
    exponent_scale,
    lengths_ref,
    order_ref,
    query_ref,
    key_hbm,
    value_hbm,
    out_ref,
    stats_ref,
    keys,
    values,
    scores,
    meta_vector,
    meta,
    block_top,
    run_top,
    run_total,
    run_out,
    by_head,
    key_sems,
    value_sems,
    meta_sem,
    when_loaded,
):
    pages, rows, head_dim = keys.shape
    seqs, heads, _ = query_ref.shape
    kv_local = rows // page_len
    shards, shard_rows, _ = out_ref.shape
    base = 2 * page_len

    def copies(hbm, buffer, sems):
        return [
            pltpu.make_async_copy(
                hbm.at[pl.ds(c * chunk, chunk)], buffer.at[pl.ds(c * chunk, chunk)], sems.at[c]
            )
            for c in range(pages // chunk)
        ]

    key_copies = copies(key_hbm, keys, key_sems)
    value_copies = copies(value_hbm, values, value_sems)
    for copy in key_copies + value_copies:
        copy.start()

    pool = order_ref.shape[0]
    order = order_ref[...].reshape(1, pool)
    rank = lax.broadcasted_iota(jnp.int32, (1, pool), 1)
    owner_row = jnp.zeros((1, pool), jnp.int32)
    limit_row = jnp.zeros((1, pool), jnp.int32)
    start = jnp.int32(0)
    for s in range(seqs):
        length = lengths_ref[s]
        reached = rank >= start
        owner_row = jnp.where(reached, s, owner_row)
        limit_row = jnp.where(reached, length + start * page_len, limit_row)
        start = start + lax.div(length + (page_len - 1), page_len)
    valid_row = jnp.clip(limit_row - rank * page_len, 0, page_len)
    packed = owner_row * base + valid_row
    local_page = lax.axis_index("seq") * pages + lax.broadcasted_iota(jnp.int32, (pages, pool), 0)
    is_page = order == local_page
    found = jnp.sum(jnp.where(is_page, packed, 0), axis=1, keepdims=True)
    found = jnp.clip(found, 0, seqs * base - 1)
    page_rank = jnp.sum(jnp.where(is_page, rank, 0), axis=1, keepdims=True)
    down = lax.broadcasted_iota(jnp.int32, (pages, LANES), 0)
    across = lax.broadcasted_iota(jnp.int32, (pages, LANES), 1)
    rank_across = jnp.sum(jnp.where(down == across, page_rank, 0), axis=0, keepdims=True)
    before = jnp.where((rank_across < page_rank) & (across < pages), 1, 0)
    place = jnp.sum(before, axis=1, keepdims=True)
    hit = place == across
    sorted_page = jnp.sum(jnp.where(hit, down, 0), axis=0, keepdims=True)
    sorted_packed = jnp.sum(jnp.where(hit, found, 0), axis=0, keepdims=True)
    sorted_page = jnp.clip(sorted_page, 0, pages - 1)
    sorted_packed = jnp.clip(sorted_packed, 0, seqs * base - 1)
    down = lax.broadcasted_iota(jnp.int32, (seqs, LANES), 0)
    across = lax.broadcasted_iota(jnp.int32, (seqs, LANES), 1)
    begun = (sorted_packed >= down * base) & (across < pages)
    ended = (sorted_packed >= (down + 1) * base) & (across < pages)
    begun = jnp.where(begun, 1, 0)
    ended = jnp.where(ended, 1, 0)
    held = jnp.sum(begun - ended, axis=1, keepdims=True)
    last = jnp.maximum(pages - 1 - jnp.sum(ended, axis=1, keepdims=True), 0)
    meta_vector[0:1] = sorted_page
    meta_vector[1:2] = sorted_packed
    meta_vector[8 : 8 + pages] = jnp.broadcast_to(found, (pages, LANES))
    meta_vector[8 + pages : 8 + pages + seqs] = jnp.where(across == 0, last, held)
    meta_copy = pltpu.make_async_copy(meta_vector, meta, meta_sem)
    meta_copy.start()

    column = lax.broadcasted_iota(jnp.int32, (heads, rows), 1)
    row_head = lax.broadcasted_iota(jnp.int32, (heads, rows), 0) // group_size
    column_limit = jnp.where(column % kv_local == row_head, column, rows)
    meta_copy.wait()

    for g in range(pages // step):
        for c in range(step // chunk):
            key_copies[g * (step // chunk) + c].wait()

        for i in range(step):
            p = g * step + i
            code = meta[8 + p, 0]
            count = lax.rem(code, base) * kv_local
            score = lax.dot_general(
                query_ref[lax.div(code, base)],
                keys[p],
                (((1,), (1,)), ((), ())),
                preferred_element_type=jnp.float32,
            )
            score = jnp.where(column_limit < count, score, MASKED)
            scores[p] = score
            block_max = jnp.maximum(jnp.max(score, axis=1, keepdims=True), FLOOR)
            block_top[p] = jnp.broadcast_to(block_max, (heads, LANES))

    def owner_at(i):
        return lax.div(meta[1, i], base)

    def kept_at(i):
        if i == 0:
            return jnp.float32(0.0)
        return jnp.where(owner_at(i) == owner_at(i - 1), 1.0, 0.0).astype(jnp.float32)

    running = jnp.full((heads, LANES), FLOOR, jnp.float32)
    for i in range(pages):
        kept = kept_at(i)
        floor = (1.0 - kept) * FLOOR
        running = jnp.maximum(running * kept + floor, block_top[meta[0, i]])
        run_top[i] = running

    for copy in value_copies:
        copy.wait()
    when_loaded()

    sum_so_far = jnp.zeros((heads, LANES), jnp.float32)
    out_so_far = jnp.zeros((heads, head_dim), jnp.float32)
    for i in range(pages):
        p = meta[0, i]
        top = run_top[meta[8 + pages + owner_at(i), 0]]
        highest = jnp.concatenate([top] * (rows // LANES), axis=1)
        weight = jnp.exp2((scores[p] - highest) * exponent_scale).astype(jnp.bfloat16)
        wide = weight.astype(jnp.float32)
        partial = wide[:, :LANES]
        for b in range(1, rows // LANES):
            partial = partial + wide[:, b * LANES : (b + 1) * LANES]
        kept = kept_at(i)
        product = jnp.dot(weight, values[p], preferred_element_type=jnp.float32)
        sum_so_far = sum_so_far * kept + partial
        out_so_far = out_so_far * kept + product
        run_total[i] = sum_so_far
        run_out[i] = out_so_far

    for s in range(seqs):
        where = pl.ds(s, heads, stride=seqs)
        at = meta[8 + pages + s, 0]
        some = meta[8 + pages + s, 1] > 0
        by_head[0, where, :] = jnp.where(some, run_out[at], 0.0)
        by_head[1, where, :] = jnp.where(some, run_top[at], FLOOR)
        total = jnp.sum(run_total[at], axis=1, keepdims=True)
        by_head[2, where, :] = jnp.broadcast_to(jnp.where(some, total, 0.0), (heads, LANES))
    out_ref[...] = by_head[0].reshape(shards, shard_rows, head_dim).astype(out_ref.dtype)
    diagonal = lax.broadcasted_iota(jnp.int32, (shard_rows, LANES), 0) == (
        lax.broadcasted_iota(jnp.int32, (shard_rows, LANES), 1)
    )
    for j in range(shards):
        for k in range(2):
            part = by_head[1 + k, j * shard_rows : (j + 1) * shard_rows, :]
            stats_ref[j, k : k + 1, :] = jnp.sum(
                jnp.where(diagonal, part, 0.0), axis=0, keepdims=True
            )


def partner(me, k, count):
    if count & (count - 1):
        return lax.rem(me + k, count)
    flipped = me + k
    bit = 1
    while bit < count:
        if k & bit:
            flipped = flipped - 2 * bit * lax.rem(lax.div(me, bit), 2)
        bit *= 2
    return flipped


def source_of(me, k, count):
    if count & (count - 1):
        return lax.rem(me + count - k, count)
    return partner(me, k, count)


def mix_kernel(
    page_len,
    group_size,
    chunk,
    step,
    exponent_scale,
    lengths_ref,
    order_ref,
    query_ref,
    key_hbm,
    value_hbm,
    weight_hbm,
    out_ref,
    keys,
    values,
    scores,
    meta_vector,
    meta,
    block_top,
    run_top,
    run_total,
    run_out,
    by_head,
    partial_ref,
    stats_ref,
    outs_in,
    stats_in,
    attended,
    weight,
    sums,
    sums_in,
    key_sems,
    value_sems,
    meta_sem,
    weight_sems,
    out_send,
    out_recv,
    stats_send,
    stats_recv,
    att_send,
    att_recv,
    sum_send,
    sum_recv,
):
    shards, shard_rows, head_dim = partial_ref.shape
    ways = sums.shape[0]
    far_first = range(shards - 1, 0, -1)
    seqs = query_ref.shape[0]
    me = lax.axis_index("seq")
    half = lax.axis_index("tensor")
    pieces = weight_sems.shape[0]
    depth = weight.shape[0] // pieces
    loads = []
    for c in range(pieces):
        part = pl.ds(c * depth, depth)
        loads.append(
            pltpu.make_async_copy(weight_hbm.at[part], weight.at[part], weight_sems.at[c])
        )

    barrier = pltpu.get_barrier_semaphore()
    for k in far_first:
        pl.semaphore_signal(
            barrier, inc=1, device_id={"seq": partner(me, k, shards)}, device_id_type=MESH
        )
    for k in range(1, ways):
        pl.semaphore_signal(
            barrier, inc=1, device_id={"tensor": lax.rem(half + k, ways)}, device_id_type=MESH
        )

    def start_loads():
        for load in loads:
            load.start()

    attend(
        page_len,
        group_size,
        chunk,
        step,
        exponent_scale,
        lengths_ref,
        order_ref,
        query_ref,
        key_hbm,
        value_hbm,
        partial_ref,
        stats_ref,
        keys,
        values,
        scores,
        meta_vector,
        meta,
        block_top,
        run_top,
        run_total,
        run_out,
        by_head,
        key_sems,
        value_sems,
        meta_sem,
        start_loads,
    )
    pl.semaphore_wait(barrier, shards + ways - 2)

    sends = []
    for k in far_first:
        peer = partner(me, k, shards)
        for source, target, send, recv in (
            (stats_ref, stats_in, stats_send, stats_recv),
            (partial_ref, outs_in, out_send, out_recv),
        ):
            copy = pltpu.make_async_remote_copy(
                src_ref=source.at[peer],
                dst_ref=target.at[k],
                send_sem=send.at[k],
                recv_sem=recv.at[k],
                device_id={"seq": peer},
                device_id_type=MESH,
            )
            copy.start()
            sends.append(copy)
    stats_in[0] = stats_ref[me]
    for copy in sends[0::2]:
        copy.wait_recv()
    tops = jnp.concatenate([stats_in[k, 0:1, :] for k in range(shards)], axis=0)
    totals = jnp.concatenate([stats_in[k, 1:2, :] for k in range(shards)], axis=0)
    factor = jnp.exp2((tops - jnp.max(tops, axis=0, keepdims=True)) * exponent_scale)
    denominator = jnp.sum(factor * totals, axis=0, keepdims=True)
    used = lax.broadcasted_iota(jnp.int32, (1, LANES), 1) < shard_rows
    share = factor / jnp.where(used, denominator, 1.0)
    diagonal = lax.broadcasted_iota(jnp.int32, (shard_rows, LANES), 0) == (
        lax.broadcasted_iota(jnp.int32, (shard_rows, LANES), 1)
    )

    def column(k):
        return jnp.sum(jnp.where(diagonal, share[k : k + 1, :], 0.0), axis=1, keepdims=True)

    columns = [column(k) for k in range(shards)]
    mine = columns[0] * partial_ref[me].astype(jnp.float32)
    for k in far_first:
        sends[2 * (shards - 1 - k) + 1].wait_recv()
        mine = mine + columns[k] * outs_in[k].astype(jnp.float32)
    attended[me] = mine.astype(jnp.bfloat16)

    gathers = []
    for k in far_first:
        copy = pltpu.make_async_remote_copy(
            src_ref=attended.at[me],
            dst_ref=attended.at[me],
            send_sem=att_send.at[k],
            recv_sem=att_recv.at[k],
            device_id={"seq": partner(me, k, shards)},
            device_id_type=MESH,
        )
        copy.start()
        gathers.append(copy)
    for load in loads:
        load.wait()

    whole_heads = shard_rows // seqs
    if shard_rows % seqs == 0:
        span = whole_heads * head_dim
        result = None
        for k in (0, *reversed(far_first)):
            source = source_of(me, k, shards)
            if k:
                pltpu.make_async_remote_copy(
                    src_ref=attended.at[source],
                    dst_ref=attended.at[source],
                    send_sem=att_send.at[k],
                    recv_sem=att_recv.at[k],
                    device_id={"seq": partner(me, k, shards)},
                    device_id_type=MESH,
                ).wait_recv()
            block = attended[source]
            left = jnp.concatenate(
                [block[h * seqs : (h + 1) * seqs] for h in range(whole_heads)], axis=1
            )
            rows = weight[pl.ds(pl.multiple_of(source * span, span), span), :]
            product = jnp.dot(left, rows, preferred_element_type=jnp.float32)
            result = product if result is None else result + product
    else:
        for k in far_first:
            gathers[shards - 1 - k].wait_recv()
        per_head = seqs // shard_rows
        result = None
        for h in range(shards // per_head):
            left = jnp.concatenate(
                [attended[h * per_head + i].astype(jnp.float32) for i in range(per_head)], axis=0
            ).astype(jnp.bfloat16)
            product = jnp.dot(
                left,
                weight[h * head_dim : (h + 1) * head_dim, :],
                preferred_element_type=jnp.float32,
            )
            result = product if result is None else result + product

    kept = seqs // ways
    for i in range(ways):
        sums[i] = result[i * kept : (i + 1) * kept]
    shares = []
    for k in range(1, ways):
        peer = lax.rem(half + k, ways)
        copy = pltpu.make_async_remote_copy(
            src_ref=sums.at[peer],
            dst_ref=sums_in.at[k - 1],
            send_sem=sum_send.at[k],
            recv_sem=sum_recv.at[k],
            device_id={"tensor": peer},
            device_id_type=MESH,
        )
        copy.start()
        shares.append(copy)
    mixed = sums[half]
    for k in range(1, ways):
        shares[k - 1].wait_recv()
        mixed = mixed + sums_in[k - 1]
    out_ref[...] = mixed.astype(out_ref.dtype)
    for copy in sends + gathers + shares:
        copy.wait_send()


def body(shards, ways, query, key_cache, value_cache, lengths, page_order, out_weight):
    pages, page_len, kv_local, head_dim = key_cache.shape
    seqs, heads, _ = query.shape
    rows = page_len * kv_local
    shard_rows = seqs * heads // shards
    depth, width = out_weight.shape
    kept = seqs // ways
    chunk = 4
    step = UNROLL
    exponent_scale = math.log2(math.e) / math.sqrt(head_dim)
    vmem = pl.BlockSpec(memory_space=pltpu.VMEM)
    smem = pl.BlockSpec(memory_space=pltpu.SMEM)
    hbm = pl.BlockSpec(memory_space=pl.ANY)
    f32, bf16 = jnp.float32, jnp.bfloat16
    dma = pltpu.SemaphoreType.DMA
    meta_rows = 8 + pages + seqs

    return pl.pallas_call(
        functools.partial(
            mix_kernel, page_len, heads // kv_local, chunk, step, exponent_scale
        ),
        out_shape=jax.ShapeDtypeStruct((kept, width), bf16),
        in_specs=[smem, vmem, vmem, hbm, hbm, hbm],
        out_specs=vmem,
        scratch_shapes=[
            pltpu.VMEM((pages, rows, head_dim), bf16),
            pltpu.VMEM((pages, rows, head_dim), bf16),
            pltpu.VMEM((pages, heads, rows), f32),
            pltpu.VMEM((meta_rows, LANES), jnp.int32),
            pltpu.SMEM((meta_rows, LANES), jnp.int32),
            pltpu.VMEM((pages, heads, LANES), f32),
            pltpu.VMEM((pages, heads, LANES), f32),
            pltpu.VMEM((pages, heads, LANES), f32),
            pltpu.VMEM((pages, heads, head_dim), f32),
            pltpu.VMEM((3, seqs * heads, LANES), f32),
            pltpu.VMEM((shards, shard_rows, head_dim), bf16),
            pltpu.VMEM((shards, 2, LANES), f32),
            pltpu.VMEM((shards, shard_rows, head_dim), bf16),
            pltpu.VMEM((shards, 2, LANES), f32),
            pltpu.VMEM((shards, shard_rows, head_dim), bf16),
            pltpu.VMEM((depth, width), bf16),
            pltpu.VMEM((ways, kept, width), f32),
            pltpu.VMEM((max(ways - 1, 1), kept, width), f32),
            dma((pages // chunk,)),
            dma((pages // chunk,)),
            dma,
            dma((8,)),
            dma((shards,)),
            dma((shards,)),
            dma((shards,)),
            dma((shards,)),
            dma((shards,)),
            dma((shards,)),
            dma((ways,)),
            dma((ways,)),
        ],
        compiler_params=pltpu.CompilerParams(collective_id=0, has_side_effects=True),
    )(
        lengths,
        page_order,
        query,
        key_cache.reshape(pages, rows, head_dim),
        value_cache.reshape(pages, rows, head_dim),
        out_weight,
    )


def solution(mesh):
    in_specs = (
        P("group", "tensor", None),
        P(("group", "seq"), None, "tensor", None),
        P(("group", "seq"), None, "tensor", None),
        P("group"),
        P("group"),
        P("tensor", "seq"),
    )
    out_specs = P(("group", "tensor"), "seq")
    step = functools.partial(body, mesh.shape["seq"], mesh.shape["tensor"])
    return jax.shard_map(step, mesh=mesh, in_specs=in_specs, out_specs=out_specs, check_vma=False)
```

```python
import functools
import math

import jax
import jax.numpy as jnp
from jax import lax
from jax.experimental import pallas as pl
from jax.experimental.pallas import tpu as pltpu
from jax.sharding import PartitionSpec as P

MASKED = -1e30
FLOOR = -1e29
LANES = 128
UNROLL = 8
HALVES = 2
MESH = pl.DeviceIdType.MESH


def attend(
    page_len,
    group_size,
    chunk,
    step,
    exponent_scale,
    lengths_ref,
    order_ref,
    query_ref,
    key_hbm,
    value_hbm,
    out_ref,
    stats_ref,
    keys,
    values,
    scores,
    meta_vector,
    meta,
    block_top,
    run_top,
    run_total,
    run_out,
    by_head,
    key_sems,
    value_sems,
    meta_sem,
    when_loaded,
    order_copy,
    query_copy,
):
    pages, rows, head_dim = keys.shape
    seqs, heads, _ = query_ref.shape
    kv_local = rows // page_len
    shards, shard_rows, _ = out_ref.shape
    base = 2 * page_len

    def copies(hbm, buffer, sems):
        return [
            pltpu.make_async_copy(
                hbm.at[pl.ds(c * chunk, chunk)], buffer.at[pl.ds(c * chunk, chunk)], sems.at[c]
            )
            for c in range(pages // chunk)
        ]

    key_copies = copies(key_hbm, keys, key_sems)
    value_copies = copies(value_hbm, values, value_sems)
    for copy in key_copies + value_copies:
        copy.start()

    order_copy.wait()
    pool = order_ref.shape[0]
    order = order_ref[...].reshape(1, pool)
    rank = lax.broadcasted_iota(jnp.int32, (1, pool), 1)
    owner_row = jnp.zeros((1, pool), jnp.int32)
    limit_row = jnp.zeros((1, pool), jnp.int32)
    start = jnp.int32(0)
    for s in range(seqs):
        length = lengths_ref[s]
        reached = rank >= start
        owner_row = jnp.where(reached, s, owner_row)
        limit_row = jnp.where(reached, length + start * page_len, limit_row)
        start = start + lax.div(length + (page_len - 1), page_len)
    valid_row = jnp.clip(limit_row - rank * page_len, 0, page_len)
    packed = owner_row * base + valid_row
    local_page = lax.axis_index("seq") * pages + lax.broadcasted_iota(jnp.int32, (pages, pool), 0)
    is_page = order == local_page
    found = jnp.sum(jnp.where(is_page, packed, 0), axis=1, keepdims=True)
    found = jnp.clip(found, 0, seqs * base - 1)
    page_rank = jnp.sum(jnp.where(is_page, rank, 0), axis=1, keepdims=True)
    down = lax.broadcasted_iota(jnp.int32, (pages, LANES), 0)
    across = lax.broadcasted_iota(jnp.int32, (pages, LANES), 1)
    rank_across = jnp.sum(jnp.where(down == across, page_rank, 0), axis=0, keepdims=True)
    before = jnp.where((rank_across < page_rank) & (across < pages), 1, 0)
    place = jnp.sum(before, axis=1, keepdims=True)
    hit = place == across
    sorted_page = jnp.sum(jnp.where(hit, down, 0), axis=0, keepdims=True)
    sorted_packed = jnp.sum(jnp.where(hit, found, 0), axis=0, keepdims=True)
    sorted_page = jnp.clip(sorted_page, 0, pages - 1)
    sorted_packed = jnp.clip(sorted_packed, 0, seqs * base - 1)
    down = lax.broadcasted_iota(jnp.int32, (seqs, LANES), 0)
    across = lax.broadcasted_iota(jnp.int32, (seqs, LANES), 1)
    begun = (sorted_packed >= down * base) & (across < pages)
    ended = (sorted_packed >= (down + 1) * base) & (across < pages)
    begun = jnp.where(begun, 1, 0)
    ended = jnp.where(ended, 1, 0)
    held = jnp.sum(begun - ended, axis=1, keepdims=True)
    last = jnp.maximum(pages - 1 - jnp.sum(ended, axis=1, keepdims=True), 0)
    meta_vector[0:1] = sorted_page
    meta_vector[1:2] = sorted_packed
    meta_vector[8 : 8 + pages] = jnp.broadcast_to(found, (pages, LANES))
    meta_vector[8 + pages : 8 + pages + seqs] = jnp.where(across == 0, last, held)
    meta_copy = pltpu.make_async_copy(meta_vector, meta, meta_sem)
    meta_copy.start()

    column = lax.broadcasted_iota(jnp.int32, (heads, rows), 1)
    row_head = lax.broadcasted_iota(jnp.int32, (heads, rows), 0) // group_size
    column_limit = jnp.where(column % kv_local == row_head, column, rows)
    meta_copy.wait()
    query_copy.wait()

    for g in range(pages // step):
        for c in range(step // chunk):
            key_copies[g * (step // chunk) + c].wait()

        for i in range(step):
            p = g * step + i
            code = meta[8 + p, 0]
            count = lax.rem(code, base) * kv_local
            score = lax.dot_general(
                query_ref[lax.div(code, base)],
                keys[p],
                (((1,), (1,)), ((), ())),
                preferred_element_type=jnp.float32,
            )
            score = jnp.where(column_limit < count, score, MASKED)
            scores[p] = score
            block_max = jnp.maximum(jnp.max(score, axis=1, keepdims=True), FLOOR)
            block_top[p] = jnp.broadcast_to(block_max, (heads, LANES))

    def owner_at(i):
        return lax.div(meta[1, i], base)

    def kept_at(i):
        if i == 0:
            return jnp.float32(0.0)
        return jnp.where(owner_at(i) == owner_at(i - 1), 1.0, 0.0).astype(jnp.float32)

    running = jnp.full((heads, LANES), FLOOR, jnp.float32)
    for i in range(pages):
        kept = kept_at(i)
        floor = (1.0 - kept) * FLOOR
        running = jnp.maximum(running * kept + floor, block_top[meta[0, i]])
        run_top[i] = running

    for copy in value_copies:
        copy.wait()
    when_loaded()

    sum_so_far = jnp.zeros((heads, LANES), jnp.float32)
    out_so_far = jnp.zeros((heads, head_dim), jnp.float32)
    for i in range(pages):
        p = meta[0, i]
        top = run_top[meta[8 + pages + owner_at(i), 0]]
        highest = jnp.concatenate([top] * (rows // LANES), axis=1)
        weight = jnp.exp2((scores[p] - highest) * exponent_scale).astype(jnp.bfloat16)
        wide = weight.astype(jnp.float32)
        partial = wide[:, :LANES]
        for b in range(1, rows // LANES):
            partial = partial + wide[:, b * LANES : (b + 1) * LANES]
        kept = kept_at(i)
        product = jnp.dot(weight, values[p], preferred_element_type=jnp.float32)
        sum_so_far = sum_so_far * kept + partial
        out_so_far = out_so_far * kept + product
        run_total[i] = sum_so_far
        run_out[i] = out_so_far

    for s in range(seqs):
        where = pl.ds(s, heads, stride=seqs)
        at = meta[8 + pages + s, 0]
        some = meta[8 + pages + s, 1] > 0
        by_head[0, where, :] = jnp.where(some, run_out[at], 0.0)
        by_head[1, where, :] = jnp.where(some, run_top[at], FLOOR)
        total = jnp.sum(run_total[at], axis=1, keepdims=True)
        by_head[2, where, :] = jnp.broadcast_to(jnp.where(some, total, 0.0), (heads, LANES))
    out_ref[...] = by_head[0].reshape(shards, shard_rows, head_dim).astype(out_ref.dtype)
    diagonal = lax.broadcasted_iota(jnp.int32, (shard_rows, LANES), 0) == (
        lax.broadcasted_iota(jnp.int32, (shard_rows, LANES), 1)
    )
    for j in range(shards):
        for k in range(2):
            part = by_head[1 + k, j * shard_rows : (j + 1) * shard_rows, :]
            stats_ref[j, k : k + 1, :] = jnp.sum(
                jnp.where(diagonal, part, 0.0), axis=0, keepdims=True
            )


def partner(me, k, count):
    if count & (count - 1):
        return lax.rem(me + k, count)
    flipped = me + k
    bit = 1
    while bit < count:
        if k & bit:
            flipped = flipped - 2 * bit * lax.rem(lax.div(me, bit), 2)
        bit *= 2
    return flipped


def source_of(me, k, count):
    if count & (count - 1):
        return lax.rem(me + count - k, count)
    return partner(me, k, count)


def mix_kernel(
    page_len,
    group_size,
    chunk,
    step,
    exponent_scale,
    lengths_ref,
    order_hbm,
    query_hbm,
    key_hbm,
    value_hbm,
    weight_hbm,
    out_ref,
    order_ref,
    query_ref,
    keys,
    values,
    scores,
    meta_vector,
    meta,
    block_top,
    run_top,
    run_total,
    run_out,
    by_head,
    partial_ref,
    stats_ref,
    outs_in,
    stats_in,
    attended,
    weight,
    sums,
    sums_in,
    key_sems,
    value_sems,
    meta_sem,
    input_sems,
    weight_sems,
    out_send,
    out_recv,
    stats_send,
    stats_recv,
    att_send,
    att_recv,
    sum_send,
    sum_recv,
):
    shards, shard_rows, head_dim = partial_ref.shape
    ways = sums.shape[0]
    far_first = range(shards - 1, 0, -1)
    seqs = query_ref.shape[0]
    me = lax.axis_index("seq")
    half = lax.axis_index("tensor")
    order_copy = pltpu.make_async_copy(order_hbm, order_ref, input_sems.at[0])
    query_copy = pltpu.make_async_copy(query_hbm, query_ref, input_sems.at[1])
    order_copy.start()
    query_copy.start()
    pieces = weight_sems.shape[0]
    depth = weight.shape[0] // pieces
    loads = []
    for c in range(pieces):
        part = pl.ds(c * depth, depth)
        loads.append(
            pltpu.make_async_copy(weight_hbm.at[part], weight.at[part], weight_sems.at[c])
        )

    barrier = pltpu.get_barrier_semaphore()
    for k in far_first:
        pl.semaphore_signal(
            barrier, inc=1, device_id={"seq": partner(me, k, shards)}, device_id_type=MESH
        )
    for k in range(1, ways):
        pl.semaphore_signal(
            barrier, inc=1, device_id={"tensor": lax.rem(half + k, ways)}, device_id_type=MESH
        )

    def start_loads():
        for load in loads:
            load.start()

    attend(
        page_len,
        group_size,
        chunk,
        step,
        exponent_scale,
        lengths_ref,
        order_ref,
        query_ref,
        key_hbm,
        value_hbm,
        partial_ref,
        stats_ref,
        keys,
        values,
        scores,
        meta_vector,
        meta,
        block_top,
        run_top,
        run_total,
        run_out,
        by_head,
        key_sems,
        value_sems,
        meta_sem,
        start_loads,
        order_copy,
        query_copy,
    )
    pl.semaphore_wait(barrier, shards + ways - 2)

    cuts = HALVES if shard_rows % (16 * HALVES) == 0 else 1
    span_rows = shard_rows // cuts
    parts = [pl.ds(h * span_rows, span_rows) for h in range(cuts)]
    stats_copies, out_copies, gathers = {}, {}, {}
    for k in far_first:
        peer = partner(me, k, shards)
        stats_copies[k] = pltpu.make_async_remote_copy(
            src_ref=stats_ref.at[peer],
            dst_ref=stats_in.at[k],
            send_sem=stats_send.at[k],
            recv_sem=stats_recv.at[k],
            device_id={"seq": peer},
            device_id_type=MESH,
        )
        stats_copies[k].start()
    for h in range(cuts):
        for k in far_first:
            peer = partner(me, k, shards)
            out_copies[h, k] = pltpu.make_async_remote_copy(
                src_ref=partial_ref.at[peer, parts[h]],
                dst_ref=outs_in.at[k, parts[h]],
                send_sem=out_send.at[h * shards + k],
                recv_sem=out_recv.at[h * shards + k],
                device_id={"seq": peer},
                device_id_type=MESH,
            )
            out_copies[h, k].start()
    stats_in[0] = stats_ref[me]
    for k in far_first:
        stats_copies[k].wait_recv()
    tops = jnp.concatenate([stats_in[k, 0:1, :] for k in range(shards)], axis=0)
    totals = jnp.concatenate([stats_in[k, 1:2, :] for k in range(shards)], axis=0)
    factor = jnp.exp2((tops - jnp.max(tops, axis=0, keepdims=True)) * exponent_scale)
    denominator = jnp.sum(factor * totals, axis=0, keepdims=True)
    used = lax.broadcasted_iota(jnp.int32, (1, LANES), 1) < shard_rows
    share = factor / jnp.where(used, denominator, 1.0)

    def column(h, k):
        diagonal = lax.broadcasted_iota(jnp.int32, (span_rows, LANES), 0) + h * span_rows == (
            lax.broadcasted_iota(jnp.int32, (span_rows, LANES), 1)
        )
        return jnp.sum(jnp.where(diagonal, share[k : k + 1, :], 0.0), axis=1, keepdims=True)

    columns = {(h, k): column(h, k) for h in range(cuts) for k in range(shards)}
    for h in range(cuts):
        mine = columns[h, 0] * partial_ref[me, parts[h], :].astype(jnp.float32)
        for k in reversed(far_first):
            out_copies[h, k].wait_recv()
            mine = mine + columns[h, k] * outs_in[k, parts[h], :].astype(jnp.float32)
        attended[me, parts[h], :] = mine.astype(jnp.bfloat16)
        for k in far_first:
            gathers[h, k] = pltpu.make_async_remote_copy(
                src_ref=attended.at[me, parts[h]],
                dst_ref=attended.at[me, parts[h]],
                send_sem=att_send.at[h * shards + k],
                recv_sem=att_recv.at[h * shards + k],
                device_id={"seq": partner(me, k, shards)},
                device_id_type=MESH,
            )
            gathers[h, k].start()
    for load in loads:
        load.wait()

    whole_heads = shard_rows // seqs
    if shard_rows % seqs == 0:
        span = whole_heads * head_dim
        result = None
        for k in (0, *reversed(far_first)):
            source = source_of(me, k, shards)
            for h in range(cuts if k else 0):
                pltpu.make_async_remote_copy(
                    src_ref=attended.at[source, parts[h]],
                    dst_ref=attended.at[source, parts[h]],
                    send_sem=att_send.at[h * shards + k],
                    recv_sem=att_recv.at[h * shards + k],
                    device_id={"seq": partner(me, k, shards)},
                    device_id_type=MESH,
                ).wait_recv()
            block = attended[source]
            left = jnp.concatenate(
                [block[h * seqs : (h + 1) * seqs] for h in range(whole_heads)], axis=1
            )
            rows = weight[pl.ds(pl.multiple_of(source * span, span), span), :]
            product = jnp.dot(left, rows, preferred_element_type=jnp.float32)
            result = product if result is None else result + product
    else:
        for k in far_first:
            gathers[0, k].wait_recv()
        per_head = seqs // shard_rows
        result = None
        for h in range(shards // per_head):
            left = jnp.concatenate(
                [attended[h * per_head + i].astype(jnp.float32) for i in range(per_head)], axis=0
            ).astype(jnp.bfloat16)
            product = jnp.dot(
                left,
                weight[h * head_dim : (h + 1) * head_dim, :],
                preferred_element_type=jnp.float32,
            )
            result = product if result is None else result + product

    kept = seqs // ways
    for i in range(ways):
        sums[i] = result[i * kept : (i + 1) * kept]
    shares = []
    for k in range(1, ways):
        peer = lax.rem(half + k, ways)
        copy = pltpu.make_async_remote_copy(
            src_ref=sums.at[peer],
            dst_ref=sums_in.at[k - 1],
            send_sem=sum_send.at[k],
            recv_sem=sum_recv.at[k],
            device_id={"tensor": peer},
            device_id_type=MESH,
        )
        copy.start()
        shares.append(copy)
    mixed = sums[half]
    for k in range(1, ways):
        shares[k - 1].wait_recv()
        mixed = mixed + sums_in[k - 1]
    out_ref[...] = mixed.astype(out_ref.dtype)
    sent = [*stats_copies.values(), *out_copies.values(), *gathers.values()]
    for copy in sent + shares:
        copy.wait_send()


def body(shards, ways, query, key_cache, value_cache, lengths, page_order, out_weight):
    pages, page_len, kv_local, head_dim = key_cache.shape
    seqs, heads, _ = query.shape
    rows = page_len * kv_local
    shard_rows = seqs * heads // shards
    depth, width = out_weight.shape
    kept = seqs // ways
    chunk = 4
    step = UNROLL
    exponent_scale = math.log2(math.e) / math.sqrt(head_dim)
    vmem = pl.BlockSpec(memory_space=pltpu.VMEM)
    smem = pl.BlockSpec(memory_space=pltpu.SMEM)
    hbm = pl.BlockSpec(memory_space=pl.ANY)
    f32, bf16 = jnp.float32, jnp.bfloat16
    dma = pltpu.SemaphoreType.DMA
    meta_rows = 8 + pages + seqs

    return pl.pallas_call(
        functools.partial(
            mix_kernel, page_len, heads // kv_local, chunk, step, exponent_scale
        ),
        out_shape=jax.ShapeDtypeStruct((kept, width), bf16),
        in_specs=[smem, hbm, hbm, hbm, hbm, hbm],
        out_specs=vmem,
        scratch_shapes=[
            pltpu.VMEM(page_order.shape, jnp.int32),
            pltpu.VMEM(query.shape, bf16),
            pltpu.VMEM((pages, rows, head_dim), bf16),
            pltpu.VMEM((pages, rows, head_dim), bf16),
            pltpu.VMEM((pages, heads, rows), f32),
            pltpu.VMEM((meta_rows, LANES), jnp.int32),
            pltpu.SMEM((meta_rows, LANES), jnp.int32),
            pltpu.VMEM((pages, heads, LANES), f32),
            pltpu.VMEM((pages, heads, LANES), f32),
            pltpu.VMEM((pages, heads, LANES), f32),
            pltpu.VMEM((pages, heads, head_dim), f32),
            pltpu.VMEM((3, seqs * heads, LANES), f32),
            pltpu.VMEM((shards, shard_rows, head_dim), bf16),
            pltpu.VMEM((shards, 2, LANES), f32),
            pltpu.VMEM((shards, shard_rows, head_dim), bf16),
            pltpu.VMEM((shards, 2, LANES), f32),
            pltpu.VMEM((shards, shard_rows, head_dim), bf16),
            pltpu.VMEM((depth, width), bf16),
            pltpu.VMEM((ways, kept, width), f32),
            pltpu.VMEM((max(ways - 1, 1), kept, width), f32),
            dma((pages // chunk,)),
            dma((pages // chunk,)),
            dma,
            dma((2,)),
            dma((8,)),
            dma((HALVES * shards,)),
            dma((HALVES * shards,)),
            dma((shards,)),
            dma((shards,)),
            dma((HALVES * shards,)),
            dma((HALVES * shards,)),
            dma((ways,)),
            dma((ways,)),
        ],
        compiler_params=pltpu.CompilerParams(collective_id=0, has_side_effects=True),
    )(
        lengths,
        page_order,
        query,
        key_cache.reshape(pages, rows, head_dim),
        value_cache.reshape(pages, rows, head_dim),
        out_weight,
    )


def solution(mesh):
    in_specs = (
        P("group", "tensor", None),
        P(("group", "seq"), None, "tensor", None),
        P(("group", "seq"), None, "tensor", None),
        P("group"),
        P("group"),
        P("tensor", "seq"),
    )
    out_specs = P(("group", "tensor"), "seq")
    step = functools.partial(body, mesh.shape["seq"], mesh.shape["tensor"])
    return jax.shard_map(step, mesh=mesh, in_specs=in_specs, out_specs=out_specs, check_vma=False)
```
